32 devices in a mesh: seq: 16 (over z, y, x), mp: 2 (over core).
Axes of the slice: x: 2, y: 2, z: 4, core: 2. Of those that a mesh axis runs over, the one named last changes fastest.
Arguments:
- encoded: bfloat16 [4096, 1152], P('seq'), may hold values from -6 to 6
- frame_tokens: int32 [16, 2], P('seq'), may hold values from 1 to 196, 256 in all within a row
- slot_owner: int32 [32], replicated, may hold values from 0 to 15, as said below
- w_in: bfloat16 [1152, 3584], P('seq', 'mp'), may hold values from -0.1875 to 0.1875
- b_in: bfloat16 [3584], P('mp'), may hold values from -3 to 3
- w_out: bfloat16 [3584, 3584], P('seq', 'mp'), may hold values from -0.09375 to 0.09375
- b_out: bfloat16 [3584], P('mp'), may hold values from -6.4 to 6.4
- norm_gain: bfloat16 [3584], replicated, may hold values from 0.5 to 1.5
- w_key: bfloat16 [3584, 512], P('seq', 'mp'), may hold values from -0.09375 to 0.09375
- b_key: bfloat16 [512], P('mp'), may hold values from -3 to 3
- w_value: bfloat16 [3584, 512], P('seq', 'mp'), may hold values from -0.09375 to 0.09375
- b_value: bfloat16 [512], P('mp'), may hold values from -3 to 3
Outputs:
- keys: bfloat16 [4096, 512], P('seq', 'mp')
- values: bfloat16 [4096, 512], P('seq', 'mp')
The draws below stay inside these ranges and needn't reach their ends.
Inputs may be any that keep to these rules, and one draw needn't show every extreme that they name: `slot_owner`: each shard index 0 to 15 appears exactly twice. `frame_tokens`: each row sums to 256.
All inputs are finite; a program needn't handle non-finite values.
Results may differ from the reference program's by a relative error of at most 0.01.
Values may be sent and summed in bfloat16 or wider, within the bound.
A program may use at most 128 MiB of HBM per device.

```python
import math
import jax
import jax.numpy as jnp
import numpy as np
from jax import lax

ENC = 1152
PHID = 3584
D = 3584
KVH = 4
HEAD = 128
TSEC = 16
PATCH = 196
TOK_DEV = 256
FR_DEV = 2
TOKENS = 4096
N_SEQ = 16


def draw_slot_owner(key, part):
    return (jax.random.permutation(key, 2 * N_SEQ) // 2).astype(jnp.int32)


def draw_b_out(key, part):
    ramp = 0.2 + 1.4 * jnp.arange(D, dtype=jnp.float32) / D
    base = jax.random.truncated_normal(key, -4.0, 4.0, (D,), jnp.float32)
    return (base * ramp).astype(jnp.bfloat16)


def level_of(own_key, shape, pieces, least, high):
    gain, own = 1.0, jax.random.fold_in(own_key, 6)
    for position, blocks in pieces:
        draws = jnp.exp(jax.random.uniform(jax.random.fold_in(own, position), (blocks,), jnp.float32, least / len(pieces), high / len(pieces)))
        gain = gain * jnp.repeat(draws, shape[position] // blocks).reshape([-1 if axis == position else 1 for axis in range(len(shape))])
    return gain


def profile(amount, total, limit, slope):
    portions = [(1 << 20) // math.isqrt(grade ** slope) + 1 for grade in range(2, amount + 1)]
    surplus, holding = total - limit - (amount - 1), [1] * (amount - 1)
    while surplus > 0:
        movable = [i for i in range(amount - 1) if holding[i] < limit]
        mass, left = sum([portions[i] for i in movable]), surplus
        for i in movable:
            more = min(limit - holding[i], max(1, left * portions[i] // mass), surplus)
            holding[i] = holding[i] + more
            surplus = surplus - more
    return np.array([limit] + holding)


def ragged(rng, count, total, bound, slope):
    if count == 2:
        one = jax.random.randint(rng, (), max(1, total - bound), min(bound, total - 1) + 1)
        return jnp.stack([one, total - one])
    sizes = jnp.asarray(profile(count, total, bound, slope), jnp.int32)
    pairs = (count - 1) // 2
    donor, receiver = sizes[1:1 + 2 * pairs:2], sizes[2:2 + 2 * pairs:2]
    margin = jnp.minimum(donor - 1, bound - receiver)
    moved = jax.random.randint(jax.random.fold_in(rng, 1), (pairs,), 0, 1 << 20) % (margin + 1)
    sizes = sizes.at[1:1 + 2 * pairs:2].set(donor - moved).at[2:2 + 2 * pairs:2].set(receiver + moved)
    return sizes[jax.random.permutation(jax.random.fold_in(rng, 2), count)]


def gaussian(own_key, shape, width, reach, split=(), kind=jnp.bfloat16):
    result = width * jax.random.normal(own_key, shape, jnp.float32)
    if split:
        result = result * level_of(own_key, shape, split, -0.22, 0.18)
    return jnp.clip(result, -reach, reach).astype(kind)


def setup_inputs(seed: int = 0) -> dict:
    streams_of = jax.random.split(jax.random.key(seed), 13)
    return {
        "encoded": gaussian(streams_of[0], (TOKENS, ENC), 1.0, 6.0, ((0, 16),)),
        "frame_tokens": jax.vmap(lambda own: ragged(own, FR_DEV, TOK_DEV, PATCH, 1))(jax.random.split(streams_of[1], N_SEQ)).reshape((N_SEQ, FR_DEV)).astype(jnp.int32),
        "slot_owner": draw_slot_owner(jax.random.fold_in(streams_of[12], 71), 0),
        "w_in": gaussian(streams_of[3], (ENC, PHID), ENC ** -0.5, 0.1875, ((0, 16), (1, 2))),
        "b_in": gaussian(streams_of[4], (PHID,), 0.5, 3.0, ((0, 2),)),
        "w_out": gaussian(streams_of[5], (PHID, D), PHID ** -0.5, 0.09375, ((0, 16), (1, 2))),
        "b_out": draw_b_out(jax.random.fold_in(streams_of[12], 71), 0),
        "norm_gain": jnp.clip(1.0 + 0.1 * jax.random.normal(streams_of[7], (D,), jnp.float32), 0.5, 1.5).astype(jnp.bfloat16),
        "w_key": gaussian(streams_of[8], (D, KVH * HEAD), D ** -0.5, 0.09375, ((0, 16), (1, 2))),
        "b_key": gaussian(streams_of[9], (KVH * HEAD,), 0.5, 3.0, ((0, 2),)),
        "w_value": gaussian(streams_of[10], (D, KVH * HEAD), D ** -0.5, 0.09375, ((0, 16), (1, 2))),
        "b_value": gaussian(streams_of[11], (KVH * HEAD,), 0.5, 3.0, ((0, 2),)),
    }


norm_eps = 1e-06
rope_base = 1000000.0

def rotate(linear, frame_ids, offsets):
    pairs = HEAD // 2
    pair_index = jnp.arange(pairs)
    inverse = jnp.power(jnp.float32(rope_base), -2.0 * pair_index.astype(jnp.float32) / HEAD)
    chosen = jnp.where(pair_index[None, :] < TSEC, frame_ids[:, None], offsets[:, None]).astype(jnp.float32)
    angles = chosen * inverse[None, :]
    cosine = jnp.cos(angles)[:, None, :]
    sine = jnp.sin(angles)[:, None, :]
    shaped = linear.reshape(linear.shape[0], -1, HEAD)
    first_half = shaped[..., :pairs]
    second_half = shaped[..., pairs:]
    turned = jnp.concatenate([first_half * cosine - second_half * sine, second_half * cosine + first_half * sine], axis=-1)
    return turned.reshape(linear.shape)

def positions(local_rows, counts):
    frame_ends = jnp.cumsum(counts)
    finished = frame_ends[None, :] <= local_rows[:, None]
    frame_local = lax.optimization_barrier(jnp.sum(finished.astype(jnp.int32), axis=1))
    frame_start = lax.optimization_barrier(jnp.sum(jnp.where(finished, counts[None, :], 0), axis=1))
    return (frame_local, local_rows - frame_start)

def reference(encoded, frame_tokens, slot_owner, w_in, b_in, w_out, b_out, norm_gain, w_key, b_key, w_value, b_value):
    frames_here = frame_tokens.shape[1]

    def encode_block(operands):
        rows_in, counts, device_number = operands
        pre = jnp.dot(rows_in, w_in, preferred_element_type=jnp.float32) + b_in.astype(jnp.float32)
        hidden = jax.nn.gelu(pre, approximate=False).astype(jnp.bfloat16)
        projected = (jnp.dot(hidden, w_out, preferred_element_type=jnp.float32) + b_out.astype(jnp.float32)).astype(jnp.bfloat16)
        wide = projected.astype(jnp.float32)
        inv_rms = lax.rsqrt(lax.optimization_barrier(jnp.mean(wide * wide, axis=1)) + norm_eps)
        normed = (wide * inv_rms[:, None] * norm_gain.astype(jnp.float32)).astype(jnp.bfloat16)
        key_linear = jnp.dot(normed, w_key, preferred_element_type=jnp.float32) + b_key.astype(jnp.float32)
        value_rows = (jnp.dot(normed, w_value, preferred_element_type=jnp.float32) + b_value.astype(jnp.float32)).astype(jnp.bfloat16)
        local_rows = jnp.arange(TOK_DEV, dtype=jnp.int32)
        frame_local, offsets = positions(local_rows, counts)
        frame_ids = device_number * frames_here + frame_local
        key_rows = rotate(key_linear, frame_ids, offsets).astype(jnp.bfloat16)
        return (key_rows, value_rows)
    blocks = encoded.reshape(N_SEQ, TOK_DEV, encoded.shape[1])
    numbers = jnp.arange(N_SEQ, dtype=jnp.int32)
    key_blocks, value_blocks = lax.map(encode_block, (blocks, frame_tokens, numbers))
    key_all = key_blocks.reshape(TOKENS, -1)
    value_all = value_blocks.reshape(TOKENS, -1)
    slot_order = jnp.argsort(slot_owner, stable=True).astype(jnp.int32)
    out_rows = jnp.arange(TOKENS, dtype=jnp.int32)
    shard = out_rows // TOK_DEV
    remain = out_rows % TOK_DEV
    source = remain // 2 * (2 * N_SEQ) + slot_order[2 * shard + remain % 2]
    return (jnp.take(key_all, source, axis=0), jnp.take(value_all, source, axis=0))
```

```python
import math

import jax
import jax.numpy as jnp
from jax import lax
from jax.sharding import PartitionSpec as P

HEAD = 128
TSEC = 16


norm_eps = 1e-06
rope_base = 1000000.0


def rotate(linear, frame_ids, offsets):
    pairs = HEAD // 2
    pair_index = jnp.arange(pairs)
    inverse = jnp.power(jnp.float32(rope_base), -2.0 * pair_index.astype(jnp.float32) / HEAD)
    chosen = jnp.where(pair_index[None, :] < TSEC, frame_ids[:, None], offsets[:, None]).astype(
        jnp.float32
    )
    angles = chosen * inverse[None, :]
    cosine = jnp.cos(angles)[:, None, :]
    sine = jnp.sin(angles)[:, None, :]
    shaped = linear.reshape(linear.shape[0], -1, HEAD)
    first_half = shaped[..., :pairs]
    second_half = shaped[..., pairs:]
    turned = jnp.concatenate(
        [first_half * cosine - second_half * sine, second_half * cosine + first_half * sine],
        axis=-1,
    )
    return turned.reshape(linear.shape)


LANES = 128


def fold(block, width):
    rows, cols = block.shape
    slots, lanes = width // LANES, cols // LANES
    pieces = slots // math.gcd(slots, lanes)
    height = rows // pieces
    tall = block.reshape(pieces, height, lanes, LANES).transpose(0, 2, 1, 3)
    tall = tall.reshape(-1, slots, height, LANES).transpose(0, 2, 1, 3)
    return tall.reshape(-1, width)


def unfold(blocks, cols):
    count, rows, width = blocks.shape
    slots, lanes = width // LANES, cols // LANES
    pieces = slots // math.gcd(slots, lanes)
    height = rows * width // (cols * pieces)
    tall = blocks.reshape(count, -1, height, slots, LANES).transpose(0, 1, 3, 2, 4)
    tall = tall.reshape(count, pieces, lanes, height, LANES).transpose(0, 1, 3, 2, 4)
    return tall.reshape(-1, cols)


def shards(
    encoded,
    frame_tokens,
    slot_owner,
    w_in,
    b_in,
    w_out,
    b_out,
    norm_gain,
    w_key,
    b_key,
    w_value,
    b_value,
):
    seq_count = lax.axis_size("seq")
    in_rows, out_rows = w_in.shape[0], w_out.shape[0]
    kv_width = w_key.shape[1] + w_value.shape[1]
    packed = jnp.concatenate(
        [w_in, w_out, fold(jnp.concatenate([w_key, w_value], axis=1), w_in.shape[1])], axis=0
    )
    whole = lax.all_gather(packed, "seq", axis=0)
    all_in = whole[:, :in_rows].reshape(-1, w_in.shape[1])
    all_out = whole[:, in_rows : in_rows + out_rows].reshape(-1, w_out.shape[1])
    all_kv = unfold(whole[:, in_rows + out_rows :], kv_width)
    own_index = lax.axis_index("seq")
    tok_rows = encoded.shape[0]
    round_span = 2 * seq_count
    rounds = tok_rows // round_span
    frames_here = frame_tokens.shape[1]
    slot_order = jnp.argsort(slot_owner, stable=True)
    pick_rows = (
        jnp.arange(rounds, dtype=jnp.int32)[None, :, None] * round_span
        + slot_order.reshape(seq_count, 1, 2)
    ).reshape(-1)
    moved = jnp.take(encoded, pick_rows, axis=0).reshape(seq_count, 2 * rounds, encoded.shape[1])
    arrived = lax.all_to_all(moved, "seq", split_axis=0, concat_axis=0, tiled=True)
    all_counts = lax.all_gather(frame_tokens, "seq", axis=0, tiled=True)
    row_block = arrived.reshape(tok_rows, encoded.shape[1])
    columns = row_block
    pre = jnp.dot(
        columns, all_in, preferred_element_type=jnp.float32
    )
    hidden_half = jax.nn.gelu(pre + b_in.astype(jnp.float32), approximate=False).astype(
        jnp.bfloat16
    )
    hidden = lax.all_gather(hidden_half, "mp", axis=1, tiled=True)
    columns = hidden
    summed = jnp.dot(
        columns,
        all_out,
        preferred_element_type=jnp.float32,
    )
    projected = (summed + b_out.astype(jnp.float32)).astype(jnp.bfloat16)
    owned_slots = lax.dynamic_slice_in_dim(slot_order, own_index * 2, 2)
    local_rows = (
        jnp.arange(rounds, dtype=jnp.int32)[:, None] * round_span + owned_slots[None, :]
    ).reshape(-1)
    frame_ends = jnp.cumsum(all_counts, axis=1)
    finished = frame_ends[:, None, :] <= local_rows[None, :, None]
    frame_local = jnp.sum(finished.astype(jnp.int32), axis=2)
    frame_start = jnp.sum(jnp.where(finished, all_counts[:, None, :], 0), axis=2)
    frame_ids = (
        jnp.arange(seq_count, dtype=jnp.int32)[:, None] * frames_here + frame_local
    ).reshape(-1)
    offsets = (local_rows[None, :] - frame_start).reshape(-1)
    frame_ids, offsets = (frame_ids, offsets)
    wide = lax.all_gather(projected, "mp", axis=1, tiled=True).astype(jnp.float32)
    inv_rms = lax.rsqrt(jnp.mean(wide * wide, axis=1) + norm_eps)
    normed = (wide * inv_rms[:, None] * norm_gain.astype(jnp.float32)).astype(jnp.bfloat16)
    both = jnp.dot(normed, all_kv, preferred_element_type=jnp.float32)
    key_linear = both[:, : w_key.shape[1]]
    value_linear = both[:, w_key.shape[1] :]
    key_rows = rotate(key_linear + b_key.astype(jnp.float32), frame_ids, offsets).astype(
        jnp.bfloat16
    )
    value_rows = (value_linear + b_value.astype(jnp.float32)).astype(jnp.bfloat16)
    return (key_rows, value_rows)


def solution(mesh):
    return jax.shard_map(
        shards,
        mesh=mesh,
        in_specs=(
            P("seq", None),
            P("seq", None),
            P(),
            P("seq", "mp"),
            P("mp"),
            P("seq", "mp"),
            P("mp"),
            P(),
            P("seq", "mp"),
            P("mp"),
            P("seq", "mp"),
            P("mp"),
        ),
        out_specs=(P("seq", "mp"), P("seq", "mp")),
        check_vma=False,
    )
```

```python
import jax
import jax.numpy as jnp
from jax import lax
from jax.sharding import PartitionSpec as P

HEAD = 128
TSEC = 16


norm_eps = 1e-06
rope_base = 1000000.0


def rotate(linear, frame_ids, offsets):
    pairs = HEAD // 2
    pair_index = jnp.arange(pairs)
    inverse = jnp.power(jnp.float32(rope_base), -2.0 * pair_index.astype(jnp.float32) / HEAD)
    chosen = jnp.where(pair_index[None, :] < TSEC, frame_ids[:, None], offsets[:, None]).astype(
        jnp.float32
    )
    angles = chosen * inverse[None, :]
    cosine = jnp.cos(angles)[:, None, :]
    sine = jnp.sin(angles)[:, None, :]
    shaped = linear.reshape(linear.shape[0], -1, HEAD)
    first_half = shaped[..., :pairs]
    second_half = shaped[..., pairs:]
    turned = jnp.concatenate(
        [first_half * cosine - second_half * sine, second_half * cosine + first_half * sine],
        axis=-1,
    )
    return turned.reshape(linear.shape)


PAIR = 2


def both(block, axis):
    other = lax.ppermute(block, axis, [(0, 1), (1, 0)])
    first = lax.axis_index(axis) == 0
    return jnp.where(first, block, other), jnp.where(first, other, block)


def swapped(zeroth, oneth, axis):
    first = lax.axis_index(axis) == 0
    kept = jnp.where(first, zeroth, oneth)
    other = lax.ppermute(jnp.where(first, oneth, zeroth), axis, [(0, 1), (1, 0)])
    return jnp.where(first, kept, other), jnp.where(first, other, kept)


def shards(
    encoded,
    frame_tokens,
    slot_owner,
    w_in,
    b_in,
    w_out,
    b_out,
    norm_gain,
    w_key,
    b_key,
    w_value,
    b_value,
):
    seq = ("o", "i")
    seq_count = lax.axis_size("o") * lax.axis_size("i")
    own_index = lax.axis_index(seq)
    pair_index = lax.axis_index("i")
    tok_rows = encoded.shape[0]
    quarter = w_in.shape[1] // PAIR
    round_span = 2 * seq_count
    rounds = tok_rows // round_span
    frames_here = frame_tokens.shape[1]

    in_rows = jnp.concatenate(swapped(w_in[:, :quarter], w_in[:, quarter:], "i"), axis=0)
    all_in = lax.all_gather(in_rows, "o", axis=0, tiled=True)
    out_rows = jnp.concatenate(swapped(w_out[:, :quarter], w_out[:, quarter:], "i"), axis=0)
    kv_rows = jnp.concatenate(both(jnp.concatenate([w_key, w_value], axis=1), "i"), axis=0)
    late = lax.all_gather(jnp.concatenate([out_rows, kv_rows], axis=1), "o", axis=0, tiled=True)

    slot_order = jnp.argsort(slot_owner, stable=True)
    pick_rows = (
        jnp.arange(rounds, dtype=jnp.int32)[None, :, None] * round_span
        + slot_order.reshape(seq_count, 1, 2)
    ).reshape(-1)
    moved = jnp.take(encoded, pick_rows, axis=0).reshape(seq_count, 2 * rounds, encoded.shape[1])
    arrived = lax.all_to_all(moved, seq, split_axis=0, concat_axis=0, tiled=True)
    all_counts = lax.all_gather(frame_tokens, seq, axis=0, tiled=True)
    arrived, all_counts = lax.optimization_barrier((arrived, all_counts))
    row_block = arrived.reshape(tok_rows, encoded.shape[1])
    columns = jnp.concatenate(both(row_block, "i"), axis=0)
    own_b_in = lax.dynamic_slice_in_dim(b_in, pair_index * quarter, quarter)
    own_b_out = lax.dynamic_slice_in_dim(b_out, pair_index * quarter, quarter)
    pre = jnp.dot(columns, all_in, preferred_element_type=jnp.float32)
    hidden = jax.nn.gelu(pre + own_b_in.astype(jnp.float32), approximate=False).astype(
        jnp.bfloat16
    )
    hidden = jnp.concatenate(both(hidden, "i"), axis=1)
    hidden = jnp.concatenate(both(hidden, "mp"), axis=1)
    summed = jnp.dot(hidden, late[:, :quarter], preferred_element_type=jnp.float32)
    projected = (summed + own_b_out.astype(jnp.float32)).astype(jnp.bfloat16)
    projected = jnp.concatenate(
        swapped(projected[:tok_rows], projected[tok_rows:], "i"), axis=1
    )
    wide = jnp.concatenate(both(projected, "mp"), axis=1).astype(jnp.float32)

    owned_slots = lax.dynamic_slice_in_dim(slot_order, own_index * 2, 2)
    local_rows = (
        jnp.arange(rounds, dtype=jnp.int32)[:, None] * round_span + owned_slots[None, :]
    ).reshape(-1)
    frame_ends = jnp.cumsum(all_counts, axis=1)
    finished = frame_ends[:, None, :] <= local_rows[None, :, None]
    frame_local = jnp.sum(finished.astype(jnp.int32), axis=2)
    frame_start = jnp.sum(jnp.where(finished, all_counts[:, None, :], 0), axis=2)
    frame_ids = (
        jnp.arange(seq_count, dtype=jnp.int32)[:, None] * frames_here + frame_local
    ).reshape(-1)
    offsets = (local_rows[None, :] - frame_start).reshape(-1)

    inv_rms = lax.rsqrt(jnp.mean(wide * wide, axis=1) + norm_eps)
    normed = (wide * inv_rms[:, None] * norm_gain.astype(jnp.float32)).astype(jnp.bfloat16)
    linear = jnp.dot(normed, late[:, quarter:], preferred_element_type=jnp.float32)
    key_linear = linear[:, : w_key.shape[1]]
    value_linear = linear[:, w_key.shape[1] :]
    key_rows = rotate(key_linear + b_key.astype(jnp.float32), frame_ids, offsets).astype(
        jnp.bfloat16
    )
    value_rows = (value_linear + b_value.astype(jnp.float32)).astype(jnp.bfloat16)
    return (key_rows, value_rows)


def solution(mesh):
    seq_count, mp_count = mesh.shape["seq"], mesh.shape["mp"]
    paired = jax.sharding.Mesh(
        mesh.devices.reshape(seq_count // PAIR, PAIR, mp_count), ("o", "i", "mp")
    )
    seq = ("o", "i")
    return jax.shard_map(
        shards,
        mesh=paired,
        in_specs=(
            P(seq, None),
            P(seq, None),
            P(),
            P(seq, "mp"),
            P("mp"),
            P(seq, "mp"),
            P("mp"),
            P(),
            P(seq, "mp"),
            P("mp"),
            P(seq, "mp"),
            P("mp"),
        ),
        out_specs=(P(seq, "mp"), P(seq, "mp")),
        check_vma=False,
    )
```

```python
import jax
import jax.numpy as jnp
from jax import lax
from jax.sharding import PartitionSpec as P

HEAD = 128
TSEC = 16


norm_eps = 1e-06
rope_base = 1000000.0


def rotate(linear, frame_ids, offsets):
    pairs = HEAD // 2
    pair_index = jnp.arange(pairs)
    inverse = jnp.power(jnp.float32(rope_base), -2.0 * pair_index.astype(jnp.float32) / HEAD)
    chosen = jnp.where(pair_index[None, :] < TSEC, frame_ids[:, None], offsets[:, None]).astype(
        jnp.float32
    )
    angles = chosen * inverse[None, :]
    cosine = jnp.cos(angles)[:, None, :]
    sine = jnp.sin(angles)[:, None, :]
    shaped = linear.reshape(linear.shape[0], -1, HEAD)
    first_half = shaped[..., :pairs]
    second_half = shaped[..., pairs:]
    turned = jnp.concatenate(
        [first_half * cosine - second_half * sine, second_half * cosine + first_half * sine],
        axis=-1,
    )
    return turned.reshape(linear.shape)


PAIR = 2
LANES = 128


def both(block, axis):
    other = lax.ppermute(block, axis, [(0, 1), (1, 0)])
    first = lax.axis_index(axis) == 0
    return jnp.where(first, block, other), jnp.where(first, other, block)


def swapped(zeroth, oneth, axis):
    first = lax.axis_index(axis) == 0
    kept = jnp.where(first, zeroth, oneth)
    other = lax.ppermute(jnp.where(first, oneth, zeroth), axis, [(0, 1), (1, 0)])
    return jnp.where(first, kept, other), jnp.where(first, other, kept)


def shards(
    encoded,
    frame_tokens,
    slot_owner,
    w_in,
    b_in,
    w_out,
    b_out,
    norm_gain,
    w_key,
    b_key,
    w_value,
    b_value,
):
    seq = ("o", "i")
    seq_count = lax.axis_size("o") * lax.axis_size("i")
    own_index = lax.axis_index(seq)
    pair_index = lax.axis_index("i")
    tok_rows = encoded.shape[0]
    quarter = w_in.shape[1] // PAIR
    round_span = 2 * seq_count
    rounds = tok_rows // round_span
    frames_here = frame_tokens.shape[1]

    out_rows = jnp.concatenate(swapped(w_out[:, :quarter], w_out[:, quarter:], "i"), axis=0)
    kv_rows = jnp.concatenate(both(jnp.concatenate([w_key, w_value], axis=1), "i"), axis=0)
    late = lax.all_gather(jnp.concatenate([out_rows, kv_rows], axis=1), "o", axis=0, tiled=True)

    slot_order = jnp.argsort(slot_owner, stable=True)
    pick_rows = (
        jnp.arange(rounds, dtype=jnp.int32)[None, :, None] * round_span
        + slot_order.reshape(seq_count, 1, 2)
    ).reshape(-1)
    moved = jnp.take(encoded, pick_rows, axis=0).reshape(seq_count, 2 * rounds, encoded.shape[1])
    counts = jnp.pad(frame_tokens[0].astype(jnp.bfloat16), (0, LANES - frames_here))
    counts = jnp.broadcast_to(counts, moved.shape[:2] + (LANES,))
    moved = jnp.concatenate([moved, counts], axis=2)
    arrived = lax.all_to_all(moved, seq, split_axis=0, concat_axis=0, tiled=True)
    all_counts = arrived[:, 0, encoded.shape[1] :][:, :frames_here].astype(jnp.int32)
    row_block = arrived[:, :, : encoded.shape[1]].reshape(tok_rows, encoded.shape[1])
    parts = jnp.stack([w_in[:, :quarter], w_in[:, quarter:]])
    parts = jnp.broadcast_to(parts[None], (lax.axis_size("o"),) + parts.shape)
    all_in = lax.all_to_all(
        parts.reshape(seq_count, -1, quarter), seq, split_axis=0, concat_axis=0, tiled=True
    ).reshape(-1, quarter)
    swap = [(0, 1), (1, 0)]
    first = pair_index == 0
    columns = jnp.concatenate([lax.ppermute(row_block, "i", swap), row_block], axis=0)
    own_b_in = lax.dynamic_slice_in_dim(b_in, pair_index * quarter, quarter)
    own_b_out = lax.dynamic_slice_in_dim(b_out, pair_index * quarter, quarter)
    pre = jnp.dot(columns, all_in, preferred_element_type=jnp.float32)
    hidden = jax.nn.gelu(pre + own_b_in.astype(jnp.float32), approximate=False).astype(
        jnp.bfloat16
    )
    other = lax.ppermute(hidden, "i", swap)
    other = jnp.concatenate([other[tok_rows:], other[:tok_rows]], axis=0)
    hidden = jnp.concatenate(
        [jnp.where(first, hidden, other), jnp.where(first, other, hidden)], axis=1
    )
    hidden = jnp.concatenate(both(hidden, "mp"), axis=1)

    def project(rows):
        summed = jnp.dot(rows, late[:, :quarter], preferred_element_type=jnp.float32)
        return (summed + own_b_out.astype(jnp.float32)).astype(jnp.bfloat16)

    got = lax.ppermute(project(hidden[:tok_rows]), "i", swap)
    kept = project(hidden[tok_rows:])
    got, kept = lax.optimization_barrier((got, kept))
    projected = jnp.concatenate([jnp.where(first, kept, got), jnp.where(first, got, kept)], axis=1)
    wide = jnp.concatenate(both(projected, "mp"), axis=1).astype(jnp.float32)

    owned_slots = lax.dynamic_slice_in_dim(slot_order, own_index * 2, 2)
    local_rows = (
        jnp.arange(rounds, dtype=jnp.int32)[:, None] * round_span + owned_slots[None, :]
    ).reshape(-1)
    frame_ends = jnp.cumsum(all_counts, axis=1)
    finished = frame_ends[:, None, :] <= local_rows[None, :, None]
    frame_local = jnp.sum(finished.astype(jnp.int32), axis=2)
    frame_start = jnp.sum(jnp.where(finished, all_counts[:, None, :], 0), axis=2)
    frame_ids = (
        jnp.arange(seq_count, dtype=jnp.int32)[:, None] * frames_here + frame_local
    ).reshape(-1)
    offsets = (local_rows[None, :] - frame_start).reshape(-1)

    inv_rms = lax.rsqrt(jnp.mean(wide * wide, axis=1) + norm_eps)
    normed = (wide * inv_rms[:, None] * norm_gain.astype(jnp.float32)).astype(jnp.bfloat16)
    linear = jnp.dot(normed, late[:, quarter:], preferred_element_type=jnp.float32)
    key_linear = linear[:, : w_key.shape[1]]
    value_linear = linear[:, w_key.shape[1] :]
    key_rows = rotate(key_linear + b_key.astype(jnp.float32), frame_ids, offsets).astype(
        jnp.bfloat16
    )
    value_rows = (value_linear + b_value.astype(jnp.float32)).astype(jnp.bfloat16)
    return (key_rows, value_rows)


def solution(mesh):
    seq_count, mp_count = mesh.shape["seq"], mesh.shape["mp"]
    paired = jax.sharding.Mesh(
        mesh.devices.reshape(seq_count // PAIR, PAIR, mp_count), ("o", "i", "mp")
    )
    seq = ("o", "i")
    return jax.shard_map(
        shards,
        mesh=paired,
        in_specs=(
            P(seq, None),
            P(seq, None),
            P(),
            P(seq, "mp"),
            P("mp"),
            P(seq, "mp"),
            P("mp"),
            P(),
            P(seq, "mp"),
            P("mp"),
            P(seq, "mp"),
            P("mp"),
        ),
        out_specs=(P(seq, "mp"), P(seq, "mp")),
        check_vma=False,
    )
```

```python
import jax
import jax.numpy as jnp
from jax import lax
from jax.sharding import PartitionSpec as P

HEAD = 128
TSEC = 16


norm_eps = 1e-06
rope_base = 1000000.0


def rotate(linear, frame_ids, offsets):
    pairs = HEAD // 2
    pair_index = jnp.arange(pairs)
    inverse = jnp.power(jnp.float32(rope_base), -2.0 * pair_index.astype(jnp.float32) / HEAD)
    chosen = jnp.where(pair_index[None, :] < TSEC, frame_ids[:, None], offsets[:, None]).astype(
        jnp.float32
    )
    angles = chosen * inverse[None, :]
    cosine = jnp.cos(angles)[:, None, :]
    sine = jnp.sin(angles)[:, None, :]
    shaped = linear.reshape(linear.shape[0], -1, HEAD)
    first_half = shaped[..., :pairs]
    second_half = shaped[..., pairs:]
    turned = jnp.concatenate(
        [first_half * cosine - second_half * sine, second_half * cosine + first_half * sine],
        axis=-1,
    )
    return turned.reshape(linear.shape)


PAIR = 2
LANES = 128


def both(block, axis):
    other = lax.ppermute(block, axis, [(0, 1), (1, 0)])
    first = lax.axis_index(axis) == 0
    return jnp.where(first, block, other), jnp.where(first, other, block)


def swapped(zeroth, oneth, axis):
    first = lax.axis_index(axis) == 0
    kept = jnp.where(first, zeroth, oneth)
    other = lax.ppermute(jnp.where(first, oneth, zeroth), axis, [(0, 1), (1, 0)])
    return jnp.where(first, kept, other), jnp.where(first, other, kept)


def shards(
    encoded,
    frame_tokens,
    slot_owner,
    w_in,
    b_in,
    w_out,
    b_out,
    norm_gain,
    w_key,
    b_key,
    w_value,
    b_value,
):
    seq = ("o", "j", "i")
    seq_count = lax.axis_size(seq)
    own_index = lax.axis_index(seq)
    pair_index = lax.axis_index("i")
    tok_rows = encoded.shape[0]
    quarter = w_in.shape[1] // PAIR
    round_span = 2 * seq_count
    rounds = tok_rows // round_span
    frames_here = frame_tokens.shape[1]

    swap = [(0, 1), (1, 0)]
    out_rows = jnp.concatenate(swapped(w_out[:, :quarter], w_out[:, quarter:], "i"), axis=0)
    in_rows = jnp.concatenate(swapped(w_in[:, :quarter], w_in[:, quarter:], "i"), axis=0)
    all_in = lax.all_gather(jnp.concatenate(both(in_rows, "j")), "o", axis=0, tiled=True)
    kv_rows = jnp.concatenate(both(jnp.concatenate([w_key, w_value], axis=1), "i"), axis=0)
    kv_rows = jnp.concatenate(both(kv_rows, "j"))
    out_rows, kv_rows = lax.optimization_barrier((out_rows, kv_rows))
    own_out = lax.all_gather(out_rows, "o", axis=0, tiled=True)
    all_kv = lax.all_gather(kv_rows, "o", axis=0, tiled=True)
    other_out = lax.ppermute(own_out, "j", swap)

    slot_order = jnp.argsort(slot_owner, stable=True)
    pick_rows = (
        jnp.arange(rounds, dtype=jnp.int32)[None, :, None] * round_span
        + slot_order.reshape(seq_count, 1, 2)
    ).reshape(-1)
    moved = jnp.take(encoded, pick_rows, axis=0).reshape(seq_count, 2 * rounds, encoded.shape[1])
    counts = jnp.pad(frame_tokens[0].astype(jnp.bfloat16), (0, LANES - frames_here))
    counts = jnp.broadcast_to(counts, moved.shape[:2] + (LANES,))
    moved = jnp.concatenate([moved, counts], axis=2)
    arrived = lax.all_to_all(moved, seq, split_axis=0, concat_axis=0, tiled=True)
    all_counts = arrived[:, 0, encoded.shape[1] :][:, :frames_here].astype(jnp.int32)
    row_block = arrived[:, :, : encoded.shape[1]].reshape(tok_rows, encoded.shape[1])
    first = pair_index == 0
    columns = jnp.concatenate([lax.ppermute(row_block, "i", swap), row_block], axis=0)
    own_b_in = lax.dynamic_slice_in_dim(b_in, pair_index * quarter, quarter)
    own_b_out = lax.dynamic_slice_in_dim(b_out, pair_index * quarter, quarter)
    pre = jnp.dot(columns, all_in, preferred_element_type=jnp.float32)
    hidden = jax.nn.gelu(pre + own_b_in.astype(jnp.float32), approximate=False).astype(
        jnp.bfloat16
    )
    other = lax.ppermute(hidden, "i", swap)
    other = jnp.concatenate([other[tok_rows:], other[:tok_rows]], axis=0)
    hidden = jnp.concatenate(
        [jnp.where(first, hidden, other), jnp.where(first, other, hidden)], axis=1
    )
    hidden = jnp.concatenate(both(hidden, "mp"), axis=1)

    zeroth = lax.axis_index("j") == 0
    units = hidden.reshape(hidden.shape[0], lax.axis_size("o"), PAIR, -1)
    own_units = jnp.where(zeroth, units[:, :, 0], units[:, :, 1]).reshape(hidden.shape[0], -1)
    other_units = jnp.where(zeroth, units[:, :, 1], units[:, :, 0]).reshape(hidden.shape[0], -1)
    early = jnp.dot(own_units, own_out, preferred_element_type=jnp.float32)
    early, other_out = lax.optimization_barrier((early, other_out))

    def project(part):
        summed = early[part] + jnp.dot(
            other_units[part], other_out, preferred_element_type=jnp.float32
        )
        return (summed + own_b_out.astype(jnp.float32)).astype(jnp.bfloat16)

    got = lax.ppermute(project(slice(None, tok_rows)), "i", swap)
    kept = project(slice(tok_rows, None))
    got, kept = lax.optimization_barrier((got, kept))
    projected = jnp.concatenate([jnp.where(first, kept, got), jnp.where(first, got, kept)], axis=1)
    wide = jnp.concatenate(both(projected, "mp"), axis=1).astype(jnp.float32)

    owned_slots = lax.dynamic_slice_in_dim(slot_order, own_index * 2, 2)
    local_rows = (
        jnp.arange(rounds, dtype=jnp.int32)[:, None] * round_span + owned_slots[None, :]
    ).reshape(-1)
    frame_ends = jnp.cumsum(all_counts, axis=1)
    finished = frame_ends[:, None, :] <= local_rows[None, :, None]
    frame_local = jnp.sum(finished.astype(jnp.int32), axis=2)
    frame_start = jnp.sum(jnp.where(finished, all_counts[:, None, :], 0), axis=2)
    frame_ids = (
        jnp.arange(seq_count, dtype=jnp.int32)[:, None] * frames_here + frame_local
    ).reshape(-1)
    offsets = (local_rows[None, :] - frame_start).reshape(-1)

    inv_rms = lax.rsqrt(jnp.mean(wide * wide, axis=1) + norm_eps)
    normed = (wide * inv_rms[:, None] * norm_gain.astype(jnp.float32)).astype(jnp.bfloat16)
    linear = jnp.dot(normed, all_kv, preferred_element_type=jnp.float32)
    key_linear = linear[:, : w_key.shape[1]]
    value_linear = linear[:, w_key.shape[1] :]
    key_rows = rotate(key_linear + b_key.astype(jnp.float32), frame_ids, offsets).astype(
        jnp.bfloat16
    )
    value_rows = (value_linear + b_value.astype(jnp.float32)).astype(jnp.bfloat16)
    return (key_rows, value_rows)


def solution(mesh):
    mp_count = mesh.shape["mp"]
    paired = jax.sharding.Mesh(
        mesh.devices.reshape(-1, PAIR, PAIR, mp_count), ("o", "j", "i", "mp")
    )
    seq = ("o", "j", "i")
    return jax.shard_map(
        shards,
        mesh=paired,
        in_specs=(
            P(seq, None),
            P(seq, None),
            P(),
            P(seq, "mp"),
            P("mp"),
            P(seq, "mp"),
            P("mp"),
            P(),
            P(seq, "mp"),
            P("mp"),
            P(seq, "mp"),
            P("mp"),
        ),
        out_specs=(P(seq, "mp"), P(seq, "mp")),
        check_vma=False,
    )
```
